32 devices in a mesh: req: 2 (over x), cand: 8 (over z, y), user: 2 (over core).
Axes of the slice: x: 2, y: 2, z: 4, core: 2. Of those that a mesh axis runs over, the one named last changes fastest.
Arguments:
- table: bfloat16 [16384, 512], P(('req', 'cand')), may hold values from -6 to 6
- hot_table: bfloat16 [256, 512], replicated, may hold values from -6 to 6
- hot_ids: int32 [256], replicated, may hold values from 0 to 16383, as said below
- hist_ids: int32 [16, 1024], P(('req', 'cand'), 'user'), may hold values from 0 to 16383, as said below
- cand_ids: int32 [16, 1024], P(('req', 'cand'), 'user'), may hold values from 0 to 16383, as said below
- w_in: bfloat16 [1, 512, 2048], replicated, may hold values from -0.25 to 0.25
- w_out: bfloat16 [1, 512, 512], replicated, may hold values from -0.25 to 0.25
- in_gain: float32 [1, 512], replicated, may hold values from 0.25 to 1.75
- attn_gain: float32 [1, 512], replicated, may hold values from 0.25 to 1.75
Outputs:
- hist_out: bfloat16 [16, 1024, 512], P(('req', 'cand'), 'user')
- cand_out: bfloat16 [16, 1024, 512], P(('req', 'cand'), 'user')
The draws below stay inside these ranges and needn't reach their ends.
Inputs may be any that keep to these rules, and one draw needn't show every extreme that they name: `hot_ids`: distinct row ids. `hist_ids`: the owner of row id g is g // 1024, the index along req and cand together with req slowest. Of the 512 items of one device, those not in hot_ids have at most 64 items with any one owner, and one owner has exactly 64 of every device's items. `cand_ids`: of the 512 candidates of one device, those not in hot_ids have at most 48 candidates with any one owner, and one owner has exactly 48 of every device's candidates.
All inputs are finite; a program needn't handle non-finite values.
Results may differ from the reference program's by a relative error of at most 0.0055.
Values may be sent and summed in bfloat16 or wider, within the bound.
A program may use at most 64 MiB of HBM per device.

```python
import jax
import jax.numpy as jnp
from jax import lax

D = 512
HEADS = 4
LAYERS = 1
HIST_DEV = 512
CAND_DEV = 512
ROWS_OWN = 1024
HOT = 256
HISTORY = 1024
CANDIDATES = 1024
REQS = 16
OWNERS = 16
TABLE_ROWS = 16384
CAP_H = 64
CAP_C = 48


def busiest_owner(key):
    return jax.random.randint(jax.random.fold_in(key, 101), (), 0, OWNERS)


def hot_list(key):
    busiest = busiest_owner(key)
    chosen = jax.random.permutation(jax.random.fold_in(key, 202), (OWNERS - 1) * ROWS_OWN)[:HOT]
    owner_of = (busiest + 1 + chosen // ROWS_OWN) % OWNERS
    return (owner_of * ROWS_OWN + chosen % ROWS_OWN).astype(jnp.int32)


def lookup_ids(key, salt, per_block, capacity, block_count):
    busiest = busiest_owner(key)
    hot_rows = hot_list(key)
    levels = jax.random.randint(jax.random.fold_in(key, 303), (OWNERS,), 0, 4)
    base_key = jax.random.fold_in(key, salt)
    slot_total = OWNERS * capacity
    slot_owner = jnp.arange(slot_total) // capacity

    def one_block(block_index):
        block_keys = jax.random.split(jax.random.fold_in(base_key, block_index), 5)
        noise = jax.random.randint(block_keys[0], (slot_total,), 0, 65536)
        scores = (levels[slot_owner] * 65536 + noise) * slot_total + jnp.arange(slot_total)
        scores = jnp.where(slot_owner == busiest, -1 - jnp.arange(slot_total), scores)
        unused, picked = lax.top_k(scores, per_block - capacity)
        owners_here = jnp.concatenate([jnp.full((capacity,), busiest, jnp.int32), slot_owner[picked].astype(jnp.int32)])
        row_numbers = jax.random.randint(block_keys[1], (per_block,), 0, ROWS_OWN)
        cold_ids = owners_here * ROWS_OWN + row_numbers
        hot_pick = hot_rows[jax.random.randint(block_keys[2], (per_block,), 0, HOT)]
        hot_flag = (jax.random.randint(block_keys[3], (per_block,), 0, 8) < 2) & (jnp.arange(per_block) >= capacity)
        row_ids = jnp.where(hot_flag, hot_pick, cold_ids).astype(jnp.int32)
        return row_ids[jax.random.permutation(block_keys[4], per_block)]
    return jax.vmap(one_block)(jnp.arange(block_count))


def draw_hot_ids(key, part):
    return hot_list(key)


def draw_hist_ids(key, part):
    block_count = REQS * HISTORY // HIST_DEV
    return lookup_ids(key, 404, HIST_DEV, CAP_H, block_count).reshape(REQS, HISTORY)


def draw_cand_ids(key, part):
    block_count = REQS * CANDIDATES // CAND_DEV
    return lookup_ids(key, 505, CAND_DEV, CAP_C, block_count).reshape(REQS, CANDIDATES)


def steps_of(own_key, shape, pieces, low, high):
    def one(position, blocks):
        heights = jax.random.uniform(jax.random.fold_in(jax.random.fold_in(own_key, 6), position), (blocks,), jnp.float32, low / len(pieces), high / len(pieces))
        return jnp.repeat(jnp.exp(heights), shape[position] // blocks).reshape((-1,) + (1,) * (len(shape) - position - 1))

    factor_of = one(*pieces[0])
    for cut in pieces[1:]:
        factor_of = factor_of * one(*cut)
    return factor_of


def bell_draw(stream_key, extent, spread, limit, cuts=(), held_as=jnp.bfloat16):
    drawn = jax.random.normal(stream_key, extent, jnp.float32) * spread
    if len(cuts) > 0:
        drawn = steps_of(stream_key, extent, cuts, -0.22, 0.18) * drawn
    return jnp.clip(drawn, min=-limit, max=limit).astype(held_as)


def setup_inputs(seed: int = 0) -> dict:
    arg_keys = jax.random.split(jax.random.key(seed), 10)
    return {
        "table": bell_draw(arg_keys[0], (TABLE_ROWS, D), 1.0, 6.0, ((0, 16),)),
        "hot_table": bell_draw(arg_keys[1], (HOT, D), 1.0, 6.0),
        "hot_ids": draw_hot_ids(jax.random.fold_in(arg_keys[9], 71), 0),
        "hist_ids": draw_hist_ids(jax.random.fold_in(arg_keys[9], 71), 0),
        "cand_ids": draw_cand_ids(jax.random.fold_in(arg_keys[9], 71), 0),
        "w_in": bell_draw(arg_keys[5], (LAYERS, D, 4 * D), D ** -0.5, 0.25),
        "w_out": bell_draw(arg_keys[6], (LAYERS, D, D), D ** -0.5, 0.25),
        "in_gain": jnp.clip(1.0 + 0.15 * jax.random.normal(arg_keys[7], (LAYERS, D), jnp.float32), 0.25, 1.75),
        "attn_gain": jnp.clip(1.0 + 0.15 * jax.random.normal(arg_keys[8], (LAYERS, D), jnp.float32), 0.25, 1.75),
    }


def norm_rows(values, scale_gain):
    centre_mean = lax.optimization_barrier(jnp.mean(values, axis=-1, keepdims=True))
    centred = values - centre_mean
    variance = lax.optimization_barrier(jnp.mean(centred * centred, axis=-1, keepdims=True))
    return centred * lax.rsqrt(variance + 1e-05) * scale_gain

def lookup_rows(row_ids, table, hot_ids, hot_table):
    hot_hit = row_ids[:, None] == hot_ids[None, :]
    is_hot = jnp.any(hot_hit, axis=1)
    hot_rows = jnp.dot(hot_hit.astype(jnp.bfloat16), hot_table, preferred_element_type=jnp.float32).astype(jnp.bfloat16)
    cold_rows = jnp.take(table, row_ids, axis=0)
    return jnp.where(is_hot[:, None], hot_rows, cold_rows)

def mix_heads(queries, keys, values, keep_mask):
    feature_count = queries.shape[1]
    head_dim = feature_count // HEADS
    query_heads = queries.astype(jnp.float32).reshape(queries.shape[0], HEADS, head_dim)
    key_heads = keys.astype(jnp.float32).reshape(keys.shape[0], HEADS, head_dim)
    value_heads = values.astype(jnp.float32).reshape(values.shape[0], HEADS, head_dim)
    scores = jnp.einsum('qhd,khd->hqk', query_heads, key_heads) * (1.0 / head_dim ** 0.5)
    weights = jnp.where(keep_mask[None], jax.nn.silu(scores), 0.0).astype(jnp.bfloat16)
    mixed = jnp.einsum('hqk,khd->qhd', weights.astype(jnp.float32), value_heads)
    return mixed.reshape(queries.shape[0], feature_count)

def reference(table, hot_table, hot_ids, hist_ids, cand_ids, w_in, w_out, in_gain, attn_gain):
    feature_count = table.shape[1]

    def one_request(id_pair):
        hist_row_ids, cand_row_ids = id_pair
        hist_x = lookup_rows(hist_row_ids, table, hot_ids, hot_table)
        cand_x = lookup_rows(cand_row_ids, table, hot_ids, hot_table)
        positions = jnp.arange(hist_row_ids.shape[0])
        causal = positions[None, :] <= positions[:, None]
        every_key = jnp.ones((cand_row_ids.shape[0], hist_row_ids.shape[0]), dtype=bool)
        for layer_index in range(LAYERS):
            weights_in = w_in[layer_index]
            hist_in = norm_rows(hist_x.astype(jnp.float32), in_gain[layer_index]).astype(jnp.bfloat16)
            cand_in = norm_rows(cand_x.astype(jnp.float32), in_gain[layer_index]).astype(jnp.bfloat16)
            projected = jax.nn.silu(jnp.dot(hist_in, weights_in, preferred_element_type=jnp.float32))
            hist_u = projected[:, :feature_count]
            hist_v = projected[:, feature_count:2 * feature_count].astype(jnp.bfloat16)
            hist_q = projected[:, 2 * feature_count:3 * feature_count].astype(jnp.bfloat16)
            hist_k = projected[:, 3 * feature_count:].astype(jnp.bfloat16)
            cand_u = jax.nn.silu(jnp.dot(cand_in, weights_in[:, :feature_count], preferred_element_type=jnp.float32))
            cand_q = jax.nn.silu(jnp.dot(cand_in, weights_in[:, 2 * feature_count:3 * feature_count], preferred_element_type=jnp.float32)).astype(jnp.bfloat16)
            hist_mix = mix_heads(hist_q, hist_k, hist_v, causal)
            cand_mix = mix_heads(cand_q, hist_k, hist_v, every_key)
            hist_gated = (norm_rows(hist_mix, attn_gain[layer_index]) * hist_u).astype(jnp.bfloat16)
            cand_gated = (norm_rows(cand_mix, attn_gain[layer_index]) * cand_u).astype(jnp.bfloat16)
            hist_x = (hist_x.astype(jnp.float32) + jnp.dot(hist_gated, w_out[layer_index], preferred_element_type=jnp.float32)).astype(jnp.bfloat16)
            cand_x = (cand_x.astype(jnp.float32) + jnp.dot(cand_gated, w_out[layer_index], preferred_element_type=jnp.float32)).astype(jnp.bfloat16)
        return (hist_x, cand_x)
    hist_out, cand_out = lax.map(one_request, (hist_ids, cand_ids))
    return (hist_out, cand_out)
```

```python
import functools

import jax
import jax.numpy as jnp
from jax import lax
from jax.experimental import pallas as pl
from jax.experimental.pallas import tpu as pltpu
from jax.sharding import PartitionSpec as P

HEADS = 4
PLANES = 4
MESH = pl.DeviceIdType.MESH
F32 = jnp.float32
BF16 = jnp.bfloat16


def round_up(value, unit):
    return -(-value // unit) * unit


def silu(values):
    half = 0.5 * values
    return half + half * jnp.tanh(half)


def norm_rows(values, scale_gain):
    centred = values - jnp.mean(values, axis=-1, keepdims=True)
    variance = jnp.mean(centred * centred, axis=-1, keepdims=True)
    return centred * lax.rsqrt(variance + 1e-05) * scale_gain


def one_hot(match):
    return jnp.where(match, 1.0, 0.0).astype(BF16)


def dot(left, right):
    return jnp.dot(left, right, preferred_element_type=F32)


def divide(ids, rows_owned):
    if rows_owned & (rows_owned - 1) == 0:
        return lax.shift_right_logical(ids, jnp.int32(rows_owned.bit_length() - 1))
    return ids // rows_owned


def place_of(owner, cands, width, members):
    req = divide(owner, cands)
    cand = owner - req * cands
    plane = divide(cand, width)
    return plane * members + req * width + cand - plane * width


def route(ids_row, hot_row, sizes, rows_owned, cap, lane_offset):
    owners, cands, width, members = sizes
    count = ids_row.shape[1]
    owner_lanes = round_up(owners, 128)
    column = jnp.transpose(jnp.broadcast_to(ids_row, (128, count)))[:, 0:1]
    hot_hit = jnp.where(column == hot_row, 1.0, 0.0)
    cold = 1.0 - jnp.max(hot_hit, axis=1, keepdims=True)
    place_column = place_of(divide(column, rows_owned), cands, width, members)
    lanes = lax.broadcasted_iota(jnp.int32, (count, owner_lanes), 1)
    member = jnp.where(place_column == lanes, cold, 0.0)
    earlier = one_hot(
        lax.broadcasted_iota(jnp.int32, (count, count), 0)
        > lax.broadcasted_iota(jnp.int32, (count, count), 1)
    )
    before = dot(earlier, member.astype(BF16))
    rank = jnp.sum(before * member, axis=1, keepdims=True).astype(jnp.int32)
    is_cold = cold > 0.5
    slot = jnp.where(is_cold, place_column * cap + rank, -1)
    lane_of = jnp.where(is_cold, rank + lane_offset, -1)
    placed = one_hot(lane_of == lax.broadcasted_iota(jnp.int32, (count, 128), 1))
    owner_row = divide(ids_row, rows_owned)
    number_row = ids_row - owner_row * rows_owned
    place_row = place_of(owner_row, cands, width, members)
    owned = place_row == lax.broadcasted_iota(jnp.int32, (owners, count), 0)
    asks = jnp.zeros((owners, 128), F32)
    scale = 1
    while scale < rows_owned:
        digit = (lax.shift_right_logical(number_row, jnp.int32(scale.bit_length() - 1)) & 255).astype(F32)
        asks = asks + float(scale) * dot(jnp.where(owned, digit, 0.0).astype(BF16), placed)
        scale *= 256
    return slot, asks.astype(jnp.int32), hot_hit.astype(BF16)


def kernel(
    sizes,
    table_hbm,
    hot_hbm,
    hot_ids_hbm,
    hist_ids_hbm,
    cand_ids_hbm,
    w_in_hbm,
    w_out_hbm,
    in_gain_hbm,
    attn_gain_hbm,
    hist_out,
    cand_out,
    hot_ids,
    hist_ids,
    cand_ids,
    in_gain,
    attn_gain,
    tables,
    hot_table,
    w_in,
    w_out,
    ask_out,
    ask_in,
    fetch_h,
    fetch_c,
    reply_h,
    reply_c,
    keys_own,
    values_own,
    keys_other,
    values_other,
    queries,
    gate_u,
    mixed,
    embedded_h,
    embedded_c,
    load_sem,
    ask_send,
    ask_recv,
    h_send,
    h_recv,
    c_send,
    c_recv,
    kv_send,
    kv_recv,
    mirror_send,
    mirror_recv,
    forward_send,
    forward_recv,
):
    reqs, cands, users, cap_h, cap_c, group, pieces = sizes
    owners = reqs * cands
    width = cands // PLANES
    members = reqs * width
    rows_owned, features = tables.shape[1:]
    head_dim = features // HEADS
    count_h = hist_ids.shape[1]
    per_source = cap_h + cap_c
    my_req = lax.axis_index("req")
    my_cand = lax.axis_index("cand")
    my_user = lax.axis_index("user")
    me = my_req * cands + my_cand
    plane = lax.div(my_cand, width)
    my_column = my_cand - plane * width
    my_member = my_req * width + my_column

    loads = [
        pltpu.make_async_copy(source, target, load_sem.at[position])
        for position, (source, target) in enumerate(
            (
                (hist_ids_hbm, hist_ids),
                (cand_ids_hbm, cand_ids),
                (hot_ids_hbm, hot_ids),
                (table_hbm, tables.at[0]),
                (hot_hbm, hot_table),
                (w_in_hbm, w_in),
                (w_out_hbm, w_out),
                (in_gain_hbm, in_gain),
                (attn_gain_hbm, attn_gain),
            )
        )
    ]
    for load in loads:
        load.start()

    barrier = pltpu.get_barrier_semaphore()

    @pl.loop(1, owners)
    def _(step):
        other = lax.rem(me + step, owners)
        other_req = lax.div(other, cands)
        pl.semaphore_signal(
            barrier,
            inc=1,
            device_id=(other_req, other - other_req * cands, my_user),
            device_id_type=MESH,
        )

    for step in range(1, users):
        pl.semaphore_signal(
            barrier,
            inc=1,
            device_id=(my_req, my_cand, lax.rem(my_user + step, users)),
            device_id_type=MESH,
        )

    inner = lax.rem(lax.div(plane + 1, 2), 2)
    outer = 1 - inner
    top = lax.div(plane, 3)
    facing = 3 - plane
    inner_side = 1 + top
    inner_far = 2 - top
    outer_side = 3 * (plane - 1)
    outer_far = 3 * (2 - plane)

    wanted = (
        (plane, plane, 0),
        (
            outer * facing + inner * outer_far,
            outer * facing + inner * outer_far,
            outer + 2 * inner,
        ),
        (
            outer * inner_far + inner * facing,
            outer * inner_side + inner * plane,
            outer + 2 * inner,
        ),
        (outer * inner_side + inner * outer_side, plane, 3),
    )

    def served(number):
        first = lax.div(3 - number, 3)
        last = lax.div(number, 3)
        second = lax.div(4 - number, 3) - first
        third = 1 - first - second - last
        middle = second + third
        source = (
            (first + outer * middle) * plane
            + inner * middle * facing
            + last * (outer * inner_side + inner * outer_side)
        )
        asker = (
            (first + last + inner * third) * plane
            + second * (outer * facing + inner * outer_side)
            + third * outer * inner_far
        )
        mirrored = last + inner * middle
        held = mirrored * (1 + lax.div(source - plane + 1, 2))
        return source, asker, held

    def member_at(step):
        req = lax.rem(my_req + lax.rem(step, reqs), reqs)
        column = lax.rem(my_column + lax.div(step, reqs), width)
        return req, column, req * width + column

    piece_rows = rows_owned // (users * pieces)

    def piece(number):
        start = pl.multiple_of((my_user * pieces + number) * piece_rows, piece_rows)
        return pl.ds(start, piece_rows)

    has_source = (plane > 0, plane < PLANES - 1)
    has_target = (plane < PLANES - 1, plane > 0)

    def mirror_copy(direction, number):
        place = direction * pieces + number
        target = lax.rem(my_cand + (width if direction == 0 else cands - width), cands)
        return pltpu.make_async_remote_copy(
            src_ref=tables.at[0, piece(number)],
            dst_ref=tables.at[1 + direction, piece(number)],
            send_sem=mirror_send.at[place],
            recv_sem=mirror_recv.at[place],
            device_id=(my_req, target, my_user),
            device_id_type=MESH,
        )

    def forward_copy(direction, number, step):
        place = (direction * pieces + number) * (users - 1) + step - 1
        return pltpu.make_async_remote_copy(
            src_ref=tables.at[1 + direction, piece(number)],
            dst_ref=tables.at[1 + direction, piece(number)],
            send_sem=forward_send.at[place],
            recv_sem=forward_recv.at[place],
            device_id=(my_req, my_cand, lax.rem(my_user + step, users)),
            device_id_type=MESH,
        )

    def ask_copy(entry, step):
        source, server, number = wanted[entry]
        req, column, member = member_at(step)
        return pltpu.make_async_remote_copy(
            src_ref=ask_out.at[source * members + member],
            dst_ref=ask_in.at[number * members + my_member],
            send_sem=ask_send.at[source * members + member],
            recv_sem=ask_recv.at[number * members + my_member],
            device_id=(req, server * width + column, my_user),
            device_id_type=MESH,
        )

    def ask_arrival(place):
        return pltpu.make_async_remote_copy(
            src_ref=ask_out.at[place],
            dst_ref=ask_in.at[place],
            send_sem=ask_send.at[place],
            recv_sem=ask_recv.at[place],
            device_id=(my_req, my_cand, my_user),
            device_id_type=MESH,
        )

    def reply_copy(number, step, fetched, replied, send_sem, recv_sem):
        source, asker, _ = served(number)
        req, column, member = member_at(step)
        return pltpu.make_async_remote_copy(
            src_ref=fetched.at[number * members + member],
            dst_ref=replied.at[source * members + my_member],
            send_sem=send_sem.at[number * members + member],
            recv_sem=recv_sem.at[source * members + my_member],
            device_id=(req, asker * width + column, my_user),
            device_id_type=MESH,
        )

    def reply_arrival(place, fetched, replied, send_sem, recv_sem):
        return pltpu.make_async_remote_copy(
            src_ref=fetched.at[place],
            dst_ref=replied.at[place],
            send_sem=send_sem.at[place],
            recv_sem=recv_sem.at[place],
            device_id=(my_req, my_cand, my_user),
            device_id_type=MESH,
        )

    hist_reply = (fetch_h, reply_h, h_send, h_recv)
    cand_reply = (fetch_c, reply_c, c_send, c_recv)

    def each_remote(other_plane, action):
        @pl.loop(0, members)
        def _(step):
            @pl.when((step > 0) | (other_plane != plane))
            def _():
                action(step)

    for load in loads[:3]:
        load.wait()
    hot_row = hot_ids[...]
    layout = (owners, cands, width, members)
    slot_h, asks_h, hot_h = route(hist_ids[...], hot_row, layout, rows_owned, cap_h, 0)
    slot_c, asks_c, hot_c = route(cand_ids[...], hot_row, layout, rows_owned, cap_c, cap_h)
    asks = asks_h + asks_c
    for owner in range(owners):
        ask_out[owner] = jnp.broadcast_to(asks[owner : owner + 1], (8, 128))
    loads[3].wait()
    pl.semaphore_wait(barrier, owners + users - 2)

    for entry in (1, 2):
        each_remote(wanted[entry][1], lambda step: ask_copy(entry, step).start())
    for number in range(pieces):
        for direction in range(2):

            @pl.when(has_target[direction])
            def _():
                mirror_copy(direction, number).start()

    for entry in (0, 3):
        each_remote(wanted[entry][1], lambda step: ask_copy(entry, step).start())

    for source, server, number in wanted:

        @pl.when(server == plane)
        def _():
            ask_in[number * members + my_member] = ask_out[source * members + my_member]

    def start_replies(number, reply):
        each_remote(
            served(number)[1], lambda step: reply_copy(number, step, *reply).start()
        )

    def serve(start, stop, reply, first, rows, ready):
        fetched, replied = reply[:2]

        @pl.loop(start, stop)
        def _(number):
            source, asker, held = served(number)

            @pl.loop(0, members // group)
            def _(turn):
                hits = []
                for item in range(group):
                    step = turn * group + item
                    place = number * members + member_at(step)[2]

                    if first == 0:

                        @pl.when((step > 0) | (asker != plane))
                        def _():
                            ask_arrival(place).wait_recv()

                    column = jnp.transpose(ask_in[place])[first : first + rows, 0:1]
                    hits.append(
                        one_hot(column == lax.broadcasted_iota(jnp.int32, (rows, rows_owned), 1))
                    )
                found = dot(jnp.concatenate(hits, axis=0), tables[held]).astype(BF16)
                for item in range(group):
                    place = number * members + member_at(turn * group + item)[2]
                    fetched[place] = found[item * rows : (item + 1) * rows]

            @pl.when(number >= ready)
            def _():
                start_replies(number, reply)

            @pl.when(asker == plane)
            def _():
                replied[source * members + my_member] = fetched[number * members + my_member]

    early = 1 + 2 * outer
    serve(0, early, hist_reply, 0, cap_h, PLANES)
    start_replies(0, hist_reply)
    serve(0, early, cand_reply, cap_h, cap_c, PLANES)
    start_replies(0, cand_reply)

    loads[4].wait()
    embedded_h[...] = dot(hot_h, hot_table[...])
    embedded_c[...] = dot(hot_c, hot_table[...])

    for number in range(pieces):
        if number == pieces - 1:
            for sent in range(pieces):
                for direction in range(2):

                    @pl.when(has_target[direction])
                    def _():
                        mirror_copy(direction, sent).wait_send()

            @pl.loop(1, early)
            def _(number):
                start_replies(number, hist_reply)

        for direction in range(2):

            @pl.when(has_source[direction])
            def _():
                mirror_copy(direction, number).wait_recv()
                for step in range(1, users):
                    forward_copy(direction, number, step).start()

    for number in range(pieces):
        for direction in range(2):
            for step in range(1, users):

                @pl.when(has_source[direction])
                def _():
                    forward_copy(direction, number, step).wait_recv()

    serve(early, PLANES, hist_reply, 0, cap_h, early)
    serve(early, PLANES, cand_reply, cap_h, cap_c, PLANES)

    for load in loads[5:]:
        load.wait()

    def gather(entries, slot, embedded, cap, arrivals):
        count = slot.shape[0]
        replied = arrivals[1]
        for entry in entries:
            source, server, _ = wanted[entry]
            offset = source * (members * cap)
            pick = one_hot(
                slot - offset == lax.broadcasted_iota(jnp.int32, (count, members * cap), 1)
            )
            each_remote(
                server,
                lambda step: reply_arrival(
                    source * members + member_at(step)[2], *arrivals
                ).wait_recv(),
            )
            rows = replied[pl.ds(source * members, members)]
            embedded[...] += dot(pick, rows.reshape(members * cap, features))

    def normed(embedded):
        return norm_rows(embedded[...], in_gain[...]).astype(BF16)

    def block(inputs, position):
        return silu(dot(inputs, w_in[:, position * features : (position + 1) * features]))

    score_scale = 1.0 / head_dim**0.5

    def attend(keys, values, mask, first):
        for head in range(HEADS):
            columns = pl.ds(head * head_dim, head_dim)
            scores = lax.dot_general(
                queries[:, columns],
                keys[:, columns],
                (((1,), (1,)), ((), ())),
                preferred_element_type=F32,
            )
            half = (scores * (0.5 * score_scale)).astype(BF16)
            weights = half + half * jnp.tanh(half)
            if mask is not None:
                weights = weights * mask
            mix = dot(weights, values[:, columns])
            if first:
                mixed[:, columns] = mix
            else:
                mixed[:, columns] += mix

    def finish(embedded):
        gated = (norm_rows(mixed[...], attn_gain[...]) * gate_u[...]).astype(BF16)
        return (embedded[...] + dot(gated, w_out[...])).astype(BF16)

    gather((0,), slot_h, embedded_h, cap_h, hist_reply)

    @pl.loop(0, PLANES)
    def _(number):
        each_remote(
            served(number)[1], lambda step: reply_copy(number, step, *hist_reply).wait_send()
        )

    @pl.loop(1, PLANES)
    def _(number):
        start_replies(number, cand_reply)

    gather((3, 2, 1), slot_h, embedded_h, cap_h, hist_reply)
    hist_in = normed(embedded_h)
    keys_own[...] = block(hist_in, 3).astype(BF16)
    values_own[...] = block(hist_in, 1).astype(BF16)
    queries[...] = block(hist_in, 2).astype(BF16)

    def kv_copies(step):
        device = (my_req, my_cand, lax.rem(my_user + step, users))
        return [
            pltpu.make_async_remote_copy(
                src_ref=source,
                dst_ref=target.at[step - 1],
                send_sem=kv_send.at[2 * (step - 1) + part],
                recv_sem=kv_recv.at[2 * (step - 1) + part],
                device_id=device,
                device_id_type=MESH,
            )
            for part, (source, target) in enumerate(
                ((keys_own, keys_other), (values_own, values_other))
            )
        ]

    sends = [copy for step in range(1, users) for copy in kv_copies(step)]
    for copy in sends:
        copy.start()
    gate_u[...] = block(hist_in, 0)
    causal = one_hot(
        lax.broadcasted_iota(jnp.int32, (count_h, count_h), 0)
        >= lax.broadcasted_iota(jnp.int32, (count_h, count_h), 1)
    )
    attend(keys_own, values_own, causal, True)
    for copy in sends:
        copy.wait_recv()
    for step in range(1, users):
        @pl.when(my_user >= step)
        def _():
            attend(keys_other.at[step - 1], values_other.at[step - 1], None, False)

    hist_out[...] = finish(embedded_h)

    gather((0, 3, 2, 1), slot_c, embedded_c, cap_c, cand_reply)
    cand_in = normed(embedded_c)
    queries[...] = block(cand_in, 2).astype(BF16)
    gate_u[...] = block(cand_in, 0)
    attend(keys_own, values_own, None, True)
    for step in range(1, users):
        attend(keys_other.at[step - 1], values_other.at[step - 1], None, False)
    cand_out[...] = finish(embedded_c)

    for entry in range(PLANES):
        each_remote(wanted[entry][1], lambda step: ask_copy(entry, step).wait_send())

    @pl.loop(0, PLANES)
    def _(number):
        asker = served(number)[1]
        each_remote(asker, lambda step: reply_copy(number, step, *cand_reply).wait_send())

    for number in range(pieces):
        for direction in range(2):

            @pl.when(has_source[direction])
            def _():
                for step in range(1, users):
                    forward_copy(direction, number, step).wait_send()

    for copy in sends:
        copy.wait_send()


def hand_out(hist_in, cand_in, hist_out, cand_out, out_sem):
    outward = [
        pltpu.make_async_copy(source, target, out_sem.at[place])
        for place, (source, target) in enumerate(((hist_in, hist_out), (cand_in, cand_out)))
    ]
    for copy in outward:
        copy.start()
    for copy in outward:
        copy.wait()


def per_device(sizes, table, hot_table, hot_ids, hist_ids, cand_ids, w_in, w_out, in_gain, attn_gain):
    reqs, cands, users = sizes
    owners = reqs * cands
    rows_owned, features = table.shape
    hot_count = hot_table.shape[0]
    count_h = hist_ids.shape[1]
    count_c = cand_ids.shape[1]
    cap_h = round_up(max(2, 2 * count_h // owners), 16)
    cap_c = round_up(max(2, 3 * count_c // (2 * owners)), 16)
    members = owners // PLANES
    group = 4 if members % 4 == 0 else 1
    pieces = 4
    vmem = pl.BlockSpec(memory_space=pltpu.VMEM)
    anywhere = pl.BlockSpec(memory_space=pl.ANY)
    dma = pltpu.SemaphoreType.DMA
    others = max(users - 1, 1)
    given = (
        table,
        hot_table,
        hot_ids[None],
        hist_ids,
        cand_ids,
        w_in[0],
        w_out[0],
        in_gain,
        attn_gain,
    )
    hist_out, cand_out = pl.pallas_call(
        functools.partial(kernel, (reqs, cands, users, cap_h, cap_c, group, pieces)),
        out_shape=(
            pltpu.VMEM((count_h, features), BF16),
            pltpu.VMEM((count_c, features), BF16),
        ),
        in_specs=[anywhere] * len(given),
        out_specs=(vmem, vmem),
        scratch_shapes=[
            pltpu.VMEM((1, hot_count), jnp.int32),
            pltpu.VMEM((1, count_h), jnp.int32),
            pltpu.VMEM((1, count_c), jnp.int32),
            pltpu.VMEM((1, features), F32),
            pltpu.VMEM((1, features), F32),
            pltpu.VMEM((3, rows_owned, features), BF16),
            pltpu.VMEM((hot_count, features), BF16),
            pltpu.VMEM((features, 4 * features), BF16),
            pltpu.VMEM((features, features), BF16),
            pltpu.VMEM((owners, 8, 128), jnp.int32),
            pltpu.VMEM((owners, 8, 128), jnp.int32),
            pltpu.VMEM((owners, cap_h, features), BF16),
            pltpu.VMEM((owners, cap_c, features), BF16),
            pltpu.VMEM((owners, cap_h, features), BF16),
            pltpu.VMEM((owners, cap_c, features), BF16),
            pltpu.VMEM((count_h, features), BF16),
            pltpu.VMEM((count_h, features), BF16),
            pltpu.VMEM((others, count_h, features), BF16),
            pltpu.VMEM((others, count_h, features), BF16),
            pltpu.VMEM((count_h, features), BF16),
            pltpu.VMEM((count_h, features), F32),
            pltpu.VMEM((count_h, features), F32),
            pltpu.VMEM((count_h, features), F32),
            pltpu.VMEM((count_c, features), F32),
            dma((len(given),)),
            dma((owners,)),
            dma((owners,)),
            dma((owners,)),
            dma((owners,)),
            dma((owners,)),
            dma((owners,)),
            dma((2 * others,)),
            dma((2 * others,)),
            dma((2 * pieces,)),
            dma((2 * pieces,)),
            dma((2 * pieces * others,)),
            dma((2 * pieces * others,)),
        ],
        compiler_params=pltpu.CompilerParams(
            collective_id=0, has_side_effects=True, vmem_limit_bytes=44 * 1024 * 1024
        ),
    )(*(pltpu.with_memory_space_constraint(array, pltpu.HBM) for array in given))
    hist_out, cand_out = pl.pallas_call(
        hand_out,
        out_shape=(
            jax.ShapeDtypeStruct((count_h, features), BF16),
            jax.ShapeDtypeStruct((count_c, features), BF16),
        ),
        in_specs=[vmem, vmem],
        out_specs=(anywhere, anywhere),
        scratch_shapes=[dma((2,))],
        compiler_params=pltpu.CompilerParams(vmem_limit_bytes=16 * 1024 * 1024),
    )(hist_out, cand_out)
    return hist_out[None], cand_out[None]


def solution(mesh):
    sizes = tuple(mesh.shape[name] for name in ("req", "cand", "user"))
    in_specs = (
        P(("req", "cand"), None),
        P(),
        P(),
        P(("req", "cand"), "user"),
        P(("req", "cand"), "user"),
        P(),
        P(),
        P(),
        P(),
    )
    out_specs = (P(("req", "cand"), "user", None), P(("req", "cand"), "user", None))
    return jax.shard_map(
        functools.partial(per_device, sizes),
        mesh=mesh,
        in_specs=in_specs,
        out_specs=out_specs,
        check_vma=False,
    )
```

```python
import functools

import jax
import jax.numpy as jnp
from jax import lax
from jax.experimental import pallas as pl
from jax.experimental.pallas import tpu as pltpu
from jax.sharding import PartitionSpec as P

HEADS = 4
PLANES = 4
MESH = pl.DeviceIdType.MESH
F32 = jnp.float32
BF16 = jnp.bfloat16


def round_up(value, unit):
    return -(-value // unit) * unit


def silu(values):
    half = 0.5 * values
    return half + half * jnp.tanh(half)


def norm_rows(values, scale_gain):
    centred = values - jnp.mean(values, axis=-1, keepdims=True)
    variance = jnp.mean(centred * centred, axis=-1, keepdims=True)
    return centred * lax.rsqrt(variance + 1e-05) * scale_gain


def one_hot(match):
    return jnp.where(match, 1.0, 0.0).astype(BF16)


def dot(left, right):
    return jnp.dot(left, right, preferred_element_type=F32)


def divide(ids, rows_owned):
    if rows_owned & (rows_owned - 1) == 0:
        return lax.shift_right_logical(ids, jnp.int32(rows_owned.bit_length() - 1))
    return ids // rows_owned


def place_of(owner, cands, width, members):
    req = divide(owner, cands)
    cand = owner - req * cands
    plane = divide(cand, width)
    return plane * members + req * width + cand - plane * width


def route(ids_row, hot_row, sizes, rows_owned, cap, lane_offset):
    owners, cands, width, members = sizes
    count = ids_row.shape[1]
    owner_lanes = round_up(owners, 128)
    column = jnp.transpose(jnp.broadcast_to(ids_row, (128, count)))[:, 0:1]
    hot_hit = jnp.where(column == hot_row, 1.0, 0.0)
    cold = 1.0 - jnp.max(hot_hit, axis=1, keepdims=True)
    place_column = place_of(divide(column, rows_owned), cands, width, members)
    lanes = lax.broadcasted_iota(jnp.int32, (count, owner_lanes), 1)
    member = jnp.where(place_column == lanes, cold, 0.0)
    earlier = one_hot(
        lax.broadcasted_iota(jnp.int32, (count, count), 0)
        > lax.broadcasted_iota(jnp.int32, (count, count), 1)
    )
    before = dot(earlier, member.astype(BF16))
    rank = jnp.sum(before * member, axis=1, keepdims=True).astype(jnp.int32)
    is_cold = cold > 0.5
    slot = jnp.where(is_cold, place_column * cap + rank, -1)
    lane_of = jnp.where(is_cold, rank + lane_offset, -1)
    placed = one_hot(lane_of == lax.broadcasted_iota(jnp.int32, (count, 128), 1))
    owner_row = divide(ids_row, rows_owned)
    number_row = ids_row - owner_row * rows_owned
    place_row = place_of(owner_row, cands, width, members)
    owned = place_row == lax.broadcasted_iota(jnp.int32, (owners, count), 0)
    asks = jnp.zeros((owners, 128), F32)
    scale = 1
    while scale < rows_owned:
        digit = (lax.shift_right_logical(number_row, jnp.int32(scale.bit_length() - 1)) & 255).astype(F32)
        asks = asks + float(scale) * dot(jnp.where(owned, digit, 0.0).astype(BF16), placed)
        scale *= 256
    return slot, asks.astype(jnp.int32), hot_hit.astype(BF16)


def kernel(
    sizes,
    table_hbm,
    hot_hbm,
    hot_ids_hbm,
    hist_ids_hbm,
    cand_ids_hbm,
    w_in_hbm,
    w_out_hbm,
    in_gain_hbm,
    attn_gain_hbm,
    hist_out,
    cand_out,
    hot_ids,
    hist_ids,
    cand_ids,
    in_gain,
    attn_gain,
    tables,
    hot_table,
    w_in,
    w_out,
    ask_out,
    ask_in,
    fetch_h,
    fetch_c,
    reply_h,
    reply_c,
    keys_own,
    values_own,
    keys_other,
    values_other,
    queries,
    gate_u,
    mixed,
    embedded_h,
    embedded_c,
    load_sem,
    ask_send,
    ask_recv,
    h_send,
    h_recv,
    c_send,
    c_recv,
    kv_send,
    kv_recv,
    mirror_send,
    mirror_recv,
    forward_send,
    forward_recv,
):
    reqs, cands, users, cap_h, cap_c, group, pieces = sizes
    owners = reqs * cands
    width = cands // PLANES
    members = reqs * width
    rows_owned, features = tables.shape[1:]
    head_dim = features // HEADS
    count_h = hist_ids.shape[1]
    per_source = cap_h + cap_c
    my_req = lax.axis_index("req")
    my_cand = lax.axis_index("cand")
    my_user = lax.axis_index("user")
    me = my_req * cands + my_cand
    plane = lax.div(my_cand, width)
    my_column = my_cand - plane * width
    my_member = my_req * width + my_column

    loads = [
        pltpu.make_async_copy(source, target, load_sem.at[position])
        for position, (source, target) in enumerate(
            (
                (hist_ids_hbm, hist_ids),
                (cand_ids_hbm, cand_ids),
                (hot_ids_hbm, hot_ids),
                (table_hbm, tables.at[0]),
                (hot_hbm, hot_table),
                (w_in_hbm, w_in),
                (w_out_hbm, w_out),
                (in_gain_hbm, in_gain),
                (attn_gain_hbm, attn_gain),
            )
        )
    ]
    for load in loads:
        load.start()

    barrier = pltpu.get_barrier_semaphore()

    @pl.loop(1, owners)
    def _(step):
        other = lax.rem(me + step, owners)
        other_req = lax.div(other, cands)
        pl.semaphore_signal(
            barrier,
            inc=1,
            device_id=(other_req, other - other_req * cands, my_user),
            device_id_type=MESH,
        )

    for step in range(1, users):
        pl.semaphore_signal(
            barrier,
            inc=1,
            device_id=(my_req, my_cand, lax.rem(my_user + step, users)),
            device_id_type=MESH,
        )

    inner = lax.rem(lax.div(plane + 1, 2), 2)
    outer = 1 - inner
    top = lax.div(plane, 3)
    facing = 3 - plane
    inner_side = 1 + top
    inner_far = 2 - top
    outer_side = 3 * (plane - 1)
    outer_far = 3 * (2 - plane)

    wanted = (
        (plane, plane, 0),
        (
            outer * facing + inner * outer_far,
            outer * facing + inner * outer_far,
            outer + 2 * inner,
        ),
        (
            outer * inner_far + inner * facing,
            outer * inner_side + inner * plane,
            outer + 2 * inner,
        ),
        (outer * inner_side + inner * outer_side, plane, 3),
    )

    def served(number):
        first = lax.div(3 - number, 3)
        last = lax.div(number, 3)
        second = lax.div(4 - number, 3) - first
        third = 1 - first - second - last
        middle = second + third
        source = (
            (first + outer * middle) * plane
            + inner * middle * facing
            + last * (outer * inner_side + inner * outer_side)
        )
        asker = (
            (first + last + inner * third) * plane
            + second * (outer * facing + inner * outer_side)
            + third * outer * inner_far
        )
        mirrored = last + inner * middle
        held = mirrored * (1 + lax.div(source - plane + 1, 2))
        return source, asker, held

    def member_at(step):
        req = lax.rem(my_req + lax.rem(step, reqs), reqs)
        column = lax.rem(my_column + lax.div(step, reqs), width)
        return req, column, req * width + column

    half_rows = rows_owned // users
    own_half = pl.multiple_of(my_user * half_rows, half_rows)
    piece_rows = half_rows // pieces

    def piece(number):
        start = pl.multiple_of((my_user * pieces + number) * piece_rows, piece_rows)
        return pl.ds(start, piece_rows)

    has_source = (plane > 0, plane < PLANES - 1)
    has_target = (plane < PLANES - 1, plane > 0)

    def mirror_copy(direction, number):
        place = direction * pieces + number
        target = lax.rem(my_cand + (width if direction == 0 else cands - width), cands)
        return pltpu.make_async_remote_copy(
            src_ref=tables.at[0, piece(number)],
            dst_ref=tables.at[1 + direction, piece(number)],
            send_sem=mirror_send.at[direction],
            recv_sem=mirror_recv.at[place],
            device_id=(my_req, target, my_user),
            device_id_type=MESH,
        )

    def forward_copy(direction, number, step):
        place = direction * (users - 1) + step - 1
        return pltpu.make_async_remote_copy(
            src_ref=tables.at[1 + direction, piece(number)],
            dst_ref=tables.at[1 + direction, piece(number)],
            send_sem=forward_send.at[place],
            recv_sem=forward_recv.at[place],
            device_id=(my_req, my_cand, lax.rem(my_user + step, users)),
            device_id_type=MESH,
        )

    def ask_copy(entry, step):
        source, server, number = wanted[entry]
        req, column, member = member_at(step)
        return pltpu.make_async_remote_copy(
            src_ref=ask_out.at[source * members + member],
            dst_ref=ask_in.at[number * members + my_member],
            send_sem=ask_send.at[0],
            recv_sem=ask_recv.at[number],
            device_id=(req, server * width + column, my_user),
            device_id_type=MESH,
        )

    def batch(held, start, count, send_sem, recv_sem):
        window = held.at[pl.ds(start, count)]
        return pltpu.make_async_remote_copy(
            src_ref=window,
            dst_ref=window,
            send_sem=send_sem,
            recv_sem=recv_sem,
            device_id=(my_req, my_cand, my_user),
            device_id_type=MESH,
        )

    def each_batch(other_plane, action):
        @pl.when(other_plane != plane)
        def _():
            action(members)

        if members > 1:

            @pl.when(other_plane == plane)
            def _():
                action(members - 1)

    def asks_arrival(number, count):
        return batch(ask_in, number * members, count, ask_send.at[0], ask_recv.at[number])

    def reply_copy(number, step, fetched, replied, send_sem, recv_sem):
        source, asker, _ = served(number)
        req, column, member = member_at(step)
        return pltpu.make_async_remote_copy(
            src_ref=fetched.at[number * members + member],
            dst_ref=replied.at[source * members + my_member],
            send_sem=send_sem.at[number],
            recv_sem=recv_sem.at[source],
            device_id=(req, asker * width + column, my_user),
            device_id_type=MESH,
        )

    def replies_sent(number, count, fetched, replied, send_sem, recv_sem):
        return batch(fetched, number * members, count, send_sem.at[number], recv_sem.at[number])

    def replies_arrival(source, count, fetched, replied, send_sem, recv_sem):
        return batch(replied, source * members, count, send_sem.at[source], recv_sem.at[source])

    hist_reply = (fetch_h, reply_h, h_send, h_recv)
    cand_reply = (fetch_c, reply_c, c_send, c_recv)

    def each_remote(other_plane, action):
        @pl.loop(0, members)
        def _(step):
            @pl.when((step > 0) | (other_plane != plane))
            def _():
                action(step)

    def start_tables(first, last):
        for number in range(first, last):
            for direction in range(2):

                @pl.when(has_target[direction])
                def _():
                    mirror_copy(direction, number).start()

    loads[3].wait()
    pl.semaphore_wait(barrier, owners + users - 2)
    start_tables(0, 1)

    for load in loads[:3]:
        load.wait()
    hot_row = hot_ids[...]
    layout = (owners, cands, width, members)
    slot_h, asks_h, hot_h = route(hist_ids[...], hot_row, layout, rows_owned, cap_h, 0)
    slot_c, asks_c, hot_c = route(cand_ids[...], hot_row, layout, rows_owned, cap_c, cap_h)
    asks = asks_h + asks_c
    for owner in range(owners):
        ask_out[owner] = jnp.broadcast_to(asks[owner : owner + 1], (8, 128))
    for entry in (1, 2):
        each_remote(wanted[entry][1], lambda step: ask_copy(entry, step).start())
    start_tables(1, pieces)
    for entry in (0, 3):
        each_remote(wanted[entry][1], lambda step: ask_copy(entry, step).start())

    for source, server, number in wanted:

        @pl.when(server == plane)
        def _():
            ask_in[number * members + my_member] = ask_out[source * members + my_member]

    def start_replies(number, reply):
        each_remote(
            served(number)[1], lambda step: reply_copy(number, step, *reply).start()
        )

    def serve(start, stop, reply, first, rows, ready):
        fetched, replied = reply[:2]

        @pl.loop(start, stop)
        def _(number):
            source, asker, held = served(number)
            if first == 0:
                each_batch(asker, lambda count: asks_arrival(number, count).wait_recv())

            @pl.loop(0, members // group)
            def _(turn):
                hits = []
                for item in range(group):
                    step = turn * group + item
                    place = number * members + member_at(step)[2]

                    column = jnp.transpose(ask_in[place])[first : first + rows, 0:1]
                    hits.append(
                        one_hot(column == lax.broadcasted_iota(jnp.int32, (rows, rows_owned), 1))
                    )
                found = dot(jnp.concatenate(hits, axis=0), tables[held]).astype(BF16)
                for item in range(group):
                    place = number * members + member_at(turn * group + item)[2]
                    fetched[place] = found[item * rows : (item + 1) * rows]

            @pl.when(number >= ready)
            def _():
                start_replies(number, reply)

            @pl.when(asker == plane)
            def _():
                replied[source * members + my_member] = fetched[number * members + my_member]

    early = 1 + 2 * outer
    serve(0, early, hist_reply, 0, cap_h, PLANES)
    start_replies(0, hist_reply)
    serve(0, early, cand_reply, cap_h, cap_c, PLANES)
    start_replies(0, cand_reply)

    loads[4].wait()
    embedded_h[...] = dot(hot_h, hot_table[...])
    embedded_c[...] = dot(hot_c, hot_table[...])

    for number in range(pieces):
        if number == pieces - 1:
            for direction in range(2):

                @pl.when(has_target[direction])
                def _():
                    batch(
                        tables.at[0], own_half, half_rows, mirror_send.at[direction], mirror_recv.at[0]
                    ).wait_send()

            @pl.loop(1, early)
            def _(number):
                start_replies(number, hist_reply)

        for direction in range(2):

            @pl.when(has_source[direction])
            def _():
                mirror_copy(direction, number).wait_recv()
                for step in range(1, users):
                    forward_copy(direction, number, step).start()

    def forwarded(direction, step):
        place = direction * (users - 1) + step - 1
        return batch(
            tables.at[1 + direction], own_half, half_rows, forward_send.at[place], forward_recv.at[place]
        )

    for direction in range(2):
        for step in range(1, users):

            @pl.when(has_source[direction])
            def _():
                forwarded(direction, step).wait_recv()

    serve(early, PLANES, hist_reply, 0, cap_h, early)
    serve(early, PLANES, cand_reply, cap_h, cap_c, PLANES)

    for load in loads[5:]:
        load.wait()

    def gather(entries, slot, embedded, cap, arrivals):
        count = slot.shape[0]
        replied = arrivals[1]
        for entry in entries:
            source, server, _ = wanted[entry]
            offset = source * (members * cap)
            pick = one_hot(
                slot - offset == lax.broadcasted_iota(jnp.int32, (count, members * cap), 1)
            )
            each_batch(
                server, lambda count: replies_arrival(source, count, *arrivals).wait_recv()
            )
            rows = replied[pl.ds(source * members, members)]
            embedded[...] += dot(pick, rows.reshape(members * cap, features))

    def normed(embedded):
        return norm_rows(embedded[...], in_gain[...]).astype(BF16)

    def block(inputs, position):
        return silu(dot(inputs, w_in[:, position * features : (position + 1) * features]))

    score_scale = 1.0 / head_dim**0.5

    def attend(keys, values, mask, first):
        for head in range(HEADS):
            columns = pl.ds(head * head_dim, head_dim)
            scores = lax.dot_general(
                queries[:, columns],
                keys[:, columns],
                (((1,), (1,)), ((), ())),
                preferred_element_type=F32,
            )
            half = (scores * (0.5 * score_scale)).astype(BF16)
            weights = half + half * jnp.tanh(half)
            if mask is not None:
                weights = weights * mask
            mix = dot(weights, values[:, columns])
            if first:
                mixed[:, columns] = mix
            else:
                mixed[:, columns] += mix

    def finish(embedded):
        gated = (norm_rows(mixed[...], attn_gain[...]) * gate_u[...]).astype(BF16)
        return (embedded[...] + dot(gated, w_out[...])).astype(BF16)

    gather((0,), slot_h, embedded_h, cap_h, hist_reply)

    @pl.loop(0, PLANES)
    def _(number):
        each_batch(
            served(number)[1], lambda count: replies_sent(number, count, *hist_reply).wait_send()
        )

    @pl.loop(1, PLANES)
    def _(number):
        start_replies(number, cand_reply)

    for local, here in ((2, outer), (3, inner)):

        @pl.when(here == 1)
        def _():
            count = PLANES * members - local
            batch(ask_out, 0, count, ask_send.at[0], ask_recv.at[0]).wait_send()

    for direction in range(2):
        for step in range(1, users):

            @pl.when(has_source[direction])
            def _():
                forwarded(direction, step).wait_send()

    gather((3, 2, 1), slot_h, embedded_h, cap_h, hist_reply)
    hist_in = normed(embedded_h)
    keys_own[...] = block(hist_in, 3).astype(BF16)
    values_own[...] = block(hist_in, 1).astype(BF16)
    queries[...] = block(hist_in, 2).astype(BF16)

    def kv_copies(step):
        device = (my_req, my_cand, lax.rem(my_user + step, users))
        return [
            pltpu.make_async_remote_copy(
                src_ref=source,
                dst_ref=target.at[step - 1],
                send_sem=kv_send.at[2 * (step - 1) + part],
                recv_sem=kv_recv.at[2 * (step - 1) + part],
                device_id=device,
                device_id_type=MESH,
            )
            for part, (source, target) in enumerate(
                ((keys_own, keys_other), (values_own, values_other))
            )
        ]

    sends = [copy for step in range(1, users) for copy in kv_copies(step)]
    for copy in sends:
        copy.start()
    gate_u[...] = block(hist_in, 0)
    causal = one_hot(
        lax.broadcasted_iota(jnp.int32, (count_h, count_h), 0)
        >= lax.broadcasted_iota(jnp.int32, (count_h, count_h), 1)
    )
    attend(keys_own, values_own, causal, True)
    for copy in sends:
        copy.wait_recv()
    for step in range(1, users):
        @pl.when(my_user >= step)
        def _():
            attend(keys_other.at[step - 1], values_other.at[step - 1], None, False)

    hist_out[...] = finish(embedded_h)

    gather((0, 3, 2, 1), slot_c, embedded_c, cap_c, cand_reply)
    cand_in = normed(embedded_c)
    queries[...] = block(cand_in, 2).astype(BF16)
    gate_u[...] = block(cand_in, 0)
    attend(keys_own, values_own, None, True)
    for step in range(1, users):
        attend(keys_other.at[step - 1], values_other.at[step - 1], None, False)
    cand_out[...] = finish(embedded_c)

    for copy in sends:
        copy.wait_send()

    @pl.loop(0, PLANES)
    def _(number):
        each_batch(
            served(number)[1], lambda count: replies_sent(number, count, *cand_reply).wait_send()
        )


def hand_out(hist_in, cand_in, hist_out, cand_out, out_sem):
    outward = [
        pltpu.make_async_copy(source, target, out_sem.at[place])
        for place, (source, target) in enumerate(((hist_in, hist_out), (cand_in, cand_out)))
    ]
    for copy in outward:
        copy.start()
    for copy in outward:
        copy.wait()


def per_device(sizes, table, hot_table, hot_ids, hist_ids, cand_ids, w_in, w_out, in_gain, attn_gain):
    reqs, cands, users = sizes
    owners = reqs * cands
    rows_owned, features = table.shape
    hot_count = hot_table.shape[0]
    count_h = hist_ids.shape[1]
    count_c = cand_ids.shape[1]
    cap_h = round_up(max(2, 2 * count_h // owners), 16)
    cap_c = round_up(max(2, 3 * count_c // (2 * owners)), 16)
    members = owners // PLANES
    group = 4 if members % 4 == 0 else 1
    pieces = 4
    vmem = pl.BlockSpec(memory_space=pltpu.VMEM)
    anywhere = pl.BlockSpec(memory_space=pl.ANY)
    dma = pltpu.SemaphoreType.DMA
    others = max(users - 1, 1)
    given = (
        table,
        hot_table,
        hot_ids[None],
        hist_ids,
        cand_ids,
        w_in[0],
        w_out[0],
        in_gain,
        attn_gain,
    )
    hist_out, cand_out = pl.pallas_call(
        functools.partial(kernel, (reqs, cands, users, cap_h, cap_c, group, pieces)),
        out_shape=(
            pltpu.VMEM((count_h, features), BF16),
            pltpu.VMEM((count_c, features), BF16),
        ),
        in_specs=[anywhere] * len(given),
        out_specs=(vmem, vmem),
        scratch_shapes=[
            pltpu.VMEM((1, hot_count), jnp.int32),
            pltpu.VMEM((1, count_h), jnp.int32),
            pltpu.VMEM((1, count_c), jnp.int32),
            pltpu.VMEM((1, features), F32),
            pltpu.VMEM((1, features), F32),
            pltpu.VMEM((3, rows_owned, features), BF16),
            pltpu.VMEM((hot_count, features), BF16),
            pltpu.VMEM((features, 4 * features), BF16),
            pltpu.VMEM((features, features), BF16),
            pltpu.VMEM((owners, 8, 128), jnp.int32),
            pltpu.VMEM((owners, 8, 128), jnp.int32),
            pltpu.VMEM((owners, cap_h, features), BF16),
            pltpu.VMEM((owners, cap_c, features), BF16),
            pltpu.VMEM((owners, cap_h, features), BF16),
            pltpu.VMEM((owners, cap_c, features), BF16),
            pltpu.VMEM((count_h, features), BF16),
            pltpu.VMEM((count_h, features), BF16),
            pltpu.VMEM((others, count_h, features), BF16),
            pltpu.VMEM((others, count_h, features), BF16),
            pltpu.VMEM((count_h, features), BF16),
            pltpu.VMEM((count_h, features), F32),
            pltpu.VMEM((count_h, features), F32),
            pltpu.VMEM((count_h, features), F32),
            pltpu.VMEM((count_c, features), F32),
            dma((len(given),)),
            dma((1,)),
            dma((PLANES,)),
            dma((PLANES,)),
            dma((PLANES,)),
            dma((PLANES,)),
            dma((PLANES,)),
            dma((2 * others,)),
            dma((2 * others,)),
            dma((2,)),
            dma((2 * pieces,)),
            dma((2 * others,)),
            dma((2 * others,)),
        ],
        compiler_params=pltpu.CompilerParams(
            collective_id=0, has_side_effects=True, vmem_limit_bytes=44 * 1024 * 1024
        ),
    )(*(pltpu.with_memory_space_constraint(array, pltpu.HBM) for array in given))
    hist_out, cand_out = pl.pallas_call(
        hand_out,
        out_shape=(
            jax.ShapeDtypeStruct((count_h, features), BF16),
            jax.ShapeDtypeStruct((count_c, features), BF16),
        ),
        in_specs=[vmem, vmem],
        out_specs=(anywhere, anywhere),
        scratch_shapes=[dma((2,))],
        compiler_params=pltpu.CompilerParams(vmem_limit_bytes=16 * 1024 * 1024),
    )(hist_out, cand_out)
    return hist_out[None], cand_out[None]


def solution(mesh):
    sizes = tuple(mesh.shape[name] for name in ("req", "cand", "user"))
    in_specs = (
        P(("req", "cand"), None),
        P(),
        P(),
        P(("req", "cand"), "user"),
        P(("req", "cand"), "user"),
        P(),
        P(),
        P(),
        P(),
    )
    out_specs = (P(("req", "cand"), "user", None), P(("req", "cand"), "user", None))
    return jax.shard_map(
        functools.partial(per_device, sizes),
        mesh=mesh,
        in_specs=in_specs,
        out_specs=out_specs,
        check_vma=False,
    )
```

```python
import functools

import jax
import jax.numpy as jnp
from jax import lax
from jax.experimental import pallas as pl
from jax.experimental.pallas import tpu as pltpu
from jax.sharding import PartitionSpec as P

HEADS = 4
PLANES = 4
MESH = pl.DeviceIdType.MESH
F32 = jnp.float32
BF16 = jnp.bfloat16


def round_up(value, unit):
    return -(-value // unit) * unit


def silu(values):
    half = 0.5 * values
    return half + half * jnp.tanh(half)


def norm_rows(values, scale_gain):
    centred = values - jnp.mean(values, axis=-1, keepdims=True)
    variance = jnp.mean(centred * centred, axis=-1, keepdims=True)
    return centred * lax.rsqrt(variance + 1e-05) * scale_gain


def one_hot(match):
    return jnp.where(match, 1.0, 0.0).astype(BF16)


def dot(left, right):
    return jnp.dot(left, right, preferred_element_type=F32)


def divide(ids, rows_owned):
    if rows_owned & (rows_owned - 1) == 0:
        return lax.shift_right_logical(ids, jnp.int32(rows_owned.bit_length() - 1))
    return ids // rows_owned


def place_of(owner, cands, width, members):
    req = divide(owner, cands)
    cand = owner - req * cands
    plane = divide(cand, width)
    return plane * members + req * width + cand - plane * width


def route(ids_row, hot_row, sizes, rows_owned, cap, lane_offset):
    owners, cands, width, members = sizes
    count = ids_row.shape[1]
    owner_lanes = round_up(owners, 128)
    column = jnp.transpose(jnp.broadcast_to(ids_row, (128, count)))[:, 0:1]
    hot_hit = jnp.where(column == hot_row, 1.0, 0.0)
    cold = 1.0 - jnp.max(hot_hit, axis=1, keepdims=True)
    place_column = place_of(divide(column, rows_owned), cands, width, members)
    lanes = lax.broadcasted_iota(jnp.int32, (count, owner_lanes), 1)
    member = jnp.where(place_column == lanes, cold, 0.0)
    earlier = one_hot(
        lax.broadcasted_iota(jnp.int32, (count, count), 0)
        > lax.broadcasted_iota(jnp.int32, (count, count), 1)
    )
    before = dot(earlier, member.astype(BF16))
    rank = jnp.sum(before * member, axis=1, keepdims=True).astype(jnp.int32)
    is_cold = cold > 0.5
    slot = jnp.where(is_cold, place_column * cap + rank, -1)
    lane_of = jnp.where(is_cold, rank + lane_offset, -1)
    placed = one_hot(lane_of == lax.broadcasted_iota(jnp.int32, (count, 128), 1))
    owner_row = divide(ids_row, rows_owned)
    number_row = ids_row - owner_row * rows_owned
    place_row = place_of(owner_row, cands, width, members)
    owned = place_row == lax.broadcasted_iota(jnp.int32, (owners, count), 0)
    asks = jnp.zeros((owners, 128), F32)
    scale = 1
    while scale < rows_owned:
        digit = (lax.shift_right_logical(number_row, jnp.int32(scale.bit_length() - 1)) & 255).astype(F32)
        asks = asks + float(scale) * dot(jnp.where(owned, digit, 0.0).astype(BF16), placed)
        scale *= 256
    return slot, asks.astype(jnp.int32), hot_hit.astype(BF16)


def kernel(
    sizes,
    table_hbm,
    hot_hbm,
    hot_ids_hbm,
    hist_ids_hbm,
    cand_ids_hbm,
    w_in_hbm,
    w_out_hbm,
    in_gain_hbm,
    attn_gain_hbm,
    hist_out,
    cand_out,
    hot_ids,
    hist_ids,
    cand_ids,
    in_gain,
    attn_gain,
    tables,
    hot_table,
    w_in,
    w_out,
    ask_out,
    ask_in,
    fetch_h,
    fetch_c,
    reply_h,
    reply_c,
    keys_own,
    values_own,
    keys_other,
    values_other,
    queries,
    gate_u,
    mixed,
    embedded_h,
    embedded_c,
    load_sem,
    ask_send,
    ask_recv,
    h_send,
    h_recv,
    c_send,
    c_recv,
    kv_send,
    kv_recv,
    mirror_send,
    mirror_recv,
    forward_send,
    forward_recv,
):
    reqs, cands, users, cap_h, cap_c, group, pieces = sizes
    owners = reqs * cands
    width = cands // PLANES
    members = reqs * width
    rows_owned, features = tables.shape[1:]
    head_dim = features // HEADS
    count_h = hist_ids.shape[1]
    per_source = cap_h + cap_c
    my_req = lax.axis_index("req")
    my_cand = lax.axis_index("cand")
    my_user = lax.axis_index("user")
    me = my_req * cands + my_cand
    plane = lax.div(my_cand, width)
    my_column = my_cand - plane * width
    my_member = my_req * width + my_column

    loads = [
        pltpu.make_async_copy(source, target, load_sem.at[position])
        for position, (source, target) in enumerate(
            (
                (hist_ids_hbm, hist_ids),
                (cand_ids_hbm, cand_ids),
                (hot_ids_hbm, hot_ids),
                (table_hbm, tables.at[0]),
                (hot_hbm, hot_table),
                (w_in_hbm, w_in),
                (w_out_hbm, w_out),
                (in_gain_hbm, in_gain),
                (attn_gain_hbm, attn_gain),
            )
        )
    ]
    for load in loads:
        load.start()

    barrier = pltpu.get_barrier_semaphore()

    @pl.loop(1, owners)
    def _(step):
        other = lax.rem(me + step, owners)
        other_req = lax.div(other, cands)
        pl.semaphore_signal(
            barrier,
            inc=1,
            device_id=(other_req, other - other_req * cands, my_user),
            device_id_type=MESH,
        )

    for step in range(1, users):
        pl.semaphore_signal(
            barrier,
            inc=1,
            device_id=(my_req, my_cand, lax.rem(my_user + step, users)),
            device_id_type=MESH,
        )

    inner = lax.rem(lax.div(plane + 1, 2), 2)
    outer = 1 - inner
    top = lax.div(plane, 3)
    facing = 3 - plane
    inner_side = 1 + top
    inner_far = 2 - top
    outer_side = 3 * (plane - 1)
    outer_far = 3 * (2 - plane)

    wanted = (
        (plane, plane, 0),
        (
            outer * facing + inner * outer_far,
            outer * facing + inner * outer_far,
            outer + 2 * inner,
        ),
        (
            outer * inner_far + inner * facing,
            outer * inner_side + inner * plane,
            outer + 2 * inner,
        ),
        (outer * inner_side + inner * outer_side, plane, 3),
    )

    def served(number):
        first = lax.div(3 - number, 3)
        last = lax.div(number, 3)
        second = lax.div(4 - number, 3) - first
        third = 1 - first - second - last
        middle = second + third
        source = (
            (first + outer * middle) * plane
            + inner * middle * facing
            + last * (outer * inner_side + inner * outer_side)
        )
        asker = (
            (first + last + inner * third) * plane
            + second * (outer * facing + inner * outer_side)
            + third * outer * inner_far
        )
        mirrored = last + inner * middle
        held = mirrored * (1 + lax.div(source - plane + 1, 2))
        return source, asker, held

    def member_at(step):
        req = lax.rem(my_req + lax.rem(step, reqs), reqs)
        column = lax.rem(my_column + lax.div(step, reqs), width)
        return req, column, req * width + column

    half_rows = rows_owned // users
    own_half = pl.multiple_of(my_user * half_rows, half_rows)
    piece_rows = half_rows // pieces

    def piece(number):
        start = pl.multiple_of((my_user * pieces + number) * piece_rows, piece_rows)
        return pl.ds(start, piece_rows)

    has_source = (plane > 0, plane < PLANES - 1)
    has_target = (plane < PLANES - 1, plane > 0)

    def mirror_copy(direction, number):
        place = direction * pieces + number
        target = lax.rem(my_cand + (width if direction == 0 else cands - width), cands)
        return pltpu.make_async_remote_copy(
            src_ref=tables.at[0, piece(number)],
            dst_ref=tables.at[1 + direction, piece(number)],
            send_sem=mirror_send.at[direction],
            recv_sem=mirror_recv.at[place],
            device_id=(my_req, target, my_user),
            device_id_type=MESH,
        )

    def forward_copy(direction, number, step):
        place = direction * (users - 1) + step - 1
        return pltpu.make_async_remote_copy(
            src_ref=tables.at[1 + direction, piece(number)],
            dst_ref=tables.at[1 + direction, piece(number)],
            send_sem=forward_send.at[place],
            recv_sem=forward_recv.at[place],
            device_id=(my_req, my_cand, lax.rem(my_user + step, users)),
            device_id_type=MESH,
        )

    def ask_copy(entry, step):
        source, server, number = wanted[entry]
        req, column, member = member_at(step)
        return pltpu.make_async_remote_copy(
            src_ref=ask_out.at[source * members + member],
            dst_ref=ask_in.at[number * members + my_member],
            send_sem=ask_send.at[0],
            recv_sem=ask_recv.at[number],
            device_id=(req, server * width + column, my_user),
            device_id_type=MESH,
        )

    def batch(held, start, count, send_sem, recv_sem):
        window = held.at[pl.ds(start, count)]
        return pltpu.make_async_remote_copy(
            src_ref=window,
            dst_ref=window,
            send_sem=send_sem,
            recv_sem=recv_sem,
            device_id=(my_req, my_cand, my_user),
            device_id_type=MESH,
        )

    def each_batch(other_plane, action):
        @pl.when(other_plane != plane)
        def _():
            action(members)

        if members > 1:

            @pl.when(other_plane == plane)
            def _():
                action(members - 1)

    def asks_arrival(number, count):
        return batch(ask_in, number * members, count, ask_send.at[0], ask_recv.at[number])

    def reply_copy(number, step, fetched, replied, send_sem, recv_sem):
        source, asker, _ = served(number)
        req, column, member = member_at(step)
        return pltpu.make_async_remote_copy(
            src_ref=fetched.at[number * members + member],
            dst_ref=replied.at[source * members + my_member],
            send_sem=send_sem.at[number],
            recv_sem=recv_sem.at[source],
            device_id=(req, asker * width + column, my_user),
            device_id_type=MESH,
        )

    def replies_sent(number, count, fetched, replied, send_sem, recv_sem):
        return batch(fetched, number * members, count, send_sem.at[number], recv_sem.at[number])

    def replies_arrival(source, count, fetched, replied, send_sem, recv_sem):
        return batch(replied, source * members, count, send_sem.at[source], recv_sem.at[source])

    hist_reply = (fetch_h, reply_h, h_send, h_recv)
    cand_reply = (fetch_c, reply_c, c_send, c_recv)

    def each_remote(other_plane, action):
        @pl.loop(0, members)
        def _(step):
            @pl.when((step > 0) | (other_plane != plane))
            def _():
                action(step)

    def start_tables(first, last):
        for number in range(first, last):
            for direction in range(2):

                @pl.when(has_target[direction])
                def _():
                    mirror_copy(direction, number).start()

    loads[3].wait()
    pl.semaphore_wait(barrier, owners + users - 2)
    start_tables(0, 1)

    for load in loads[:3]:
        load.wait()
    hot_row = hot_ids[...]
    layout = (owners, cands, width, members)
    slot_h, asks_h, hot_h = route(hist_ids[...], hot_row, layout, rows_owned, cap_h, 0)
    slot_c, asks_c, hot_c = route(cand_ids[...], hot_row, layout, rows_owned, cap_c, cap_h)
    asks = asks_h + asks_c
    for owner in range(owners):
        ask_out[owner] = jnp.broadcast_to(asks[owner : owner + 1], (8, 128))
    for entry in (1, 2):
        each_remote(wanted[entry][1], lambda step: ask_copy(entry, step).start())
    start_tables(1, pieces)
    for entry in (0, 3):
        each_remote(wanted[entry][1], lambda step: ask_copy(entry, step).start())

    for source, server, number in wanted:

        @pl.when(server == plane)
        def _():
            ask_in[number * members + my_member] = ask_out[source * members + my_member]

    def start_replies(number, reply):
        each_remote(
            served(number)[1], lambda step: reply_copy(number, step, *reply).start()
        )

    def serve(start, stop, reply, first, rows, ready):
        fetched, replied = reply[:2]

        @pl.loop(start, stop)
        def _(number):
            source, asker, held = served(number)
            if first == 0:
                each_batch(asker, lambda count: asks_arrival(number, count).wait_recv())

            @pl.loop(0, members // group)
            def _(turn):
                hits = []
                for item in range(group):
                    step = turn * group + item
                    place = number * members + member_at(step)[2]

                    column = jnp.transpose(ask_in[place])[first : first + rows, 0:1]
                    hits.append(
                        one_hot(column == lax.broadcasted_iota(jnp.int32, (rows, rows_owned), 1))
                    )
                found = dot(jnp.concatenate(hits, axis=0), tables[held]).astype(BF16)
                for item in range(group):
                    place = number * members + member_at(turn * group + item)[2]
                    fetched[place] = found[item * rows : (item + 1) * rows]

            @pl.when(number >= ready)
            def _():
                start_replies(number, reply)

            @pl.when(asker == plane)
            def _():
                replied[source * members + my_member] = fetched[number * members + my_member]

    early = 1 + 2 * outer
    serve(0, early, hist_reply, 0, cap_h, PLANES)
    start_replies(0, hist_reply)
    serve(0, early, cand_reply, cap_h, cap_c, PLANES)
    start_replies(0, cand_reply)

    loads[4].wait()
    embedded_h[...] = dot(hot_h, hot_table[...])
    embedded_c[...] = dot(hot_c, hot_table[...])

    for number in range(pieces):
        if number == pieces - 1:
            for direction in range(2):

                @pl.when(has_target[direction])
                def _():
                    batch(
                        tables.at[0], own_half, half_rows, mirror_send.at[direction], mirror_recv.at[0]
                    ).wait_send()

            @pl.loop(1, early)
            def _(number):
                start_replies(number, hist_reply)

        for direction in range(2):

            @pl.when(has_source[direction])
            def _():
                mirror_copy(direction, number).wait_recv()
                for step in range(1, users):
                    forward_copy(direction, number, step).start()

    def forwarded(direction, step):
        place = direction * (users - 1) + step - 1
        return batch(
            tables.at[1 + direction], own_half, half_rows, forward_send.at[place], forward_recv.at[place]
        )

    for direction in range(2):
        for step in range(1, users):

            @pl.when(has_source[direction])
            def _():
                forwarded(direction, step).wait_recv()

    serve(early, PLANES, hist_reply, 0, cap_h, early)
    serve(early, PLANES, cand_reply, cap_h, cap_c, PLANES)

    for load in loads[5:]:
        load.wait()

    def gather(entries, slot, embedded, cap, arrivals):
        count = slot.shape[0]
        replied = arrivals[1]
        for entry in entries:
            source, server, _ = wanted[entry]
            offset = source * (members * cap)
            pick = one_hot(
                slot - offset == lax.broadcasted_iota(jnp.int32, (count, members * cap), 1)
            )
            each_batch(
                server, lambda count: replies_arrival(source, count, *arrivals).wait_recv()
            )
            rows = replied[pl.ds(source * members, members)]
            embedded[...] += dot(pick, rows.reshape(members * cap, features))

    def normed(embedded):
        return norm_rows(embedded[...], in_gain[...]).astype(BF16)

    def block(inputs, position):
        return silu(dot(inputs, w_in[:, position * features : (position + 1) * features]))

    score_scale = 1.0 / head_dim**0.5

    def attend(keys, values, mask, first, rows=slice(None), kept=slice(None)):
        for head in range(HEADS):
            columns = pl.ds(head * head_dim, head_dim)
            scores = lax.dot_general(
                queries[rows, columns],
                keys[kept, columns],
                (((1,), (1,)), ((), ())),
                preferred_element_type=F32,
            )
            half = (scores * (0.5 * score_scale)).astype(BF16)
            weights = half + half * jnp.tanh(half)
            if mask is not None:
                weights = weights * mask
            mix = dot(weights, values[kept, columns])
            if first:
                mixed[rows, columns] = mix
            else:
                mixed[rows, columns] += mix

    def finish(embedded):
        gated = (norm_rows(mixed[...], attn_gain[...]) * gate_u[...]).astype(BF16)
        return (embedded[...] + dot(gated, w_out[...])).astype(BF16)

    gather((0,), slot_h, embedded_h, cap_h, hist_reply)

    @pl.loop(0, PLANES)
    def _(number):
        each_batch(
            served(number)[1], lambda count: replies_sent(number, count, *hist_reply).wait_send()
        )

    @pl.loop(1, PLANES)
    def _(number):
        start_replies(number, cand_reply)

    for local, here in ((2, outer), (3, inner)):

        @pl.when(here == 1)
        def _():
            count = PLANES * members - local
            batch(ask_out, 0, count, ask_send.at[0], ask_recv.at[0]).wait_send()

    for direction in range(2):
        for step in range(1, users):

            @pl.when(has_source[direction])
            def _():
                forwarded(direction, step).wait_send()

    gather((3, 2, 1), slot_h, embedded_h, cap_h, hist_reply)
    hist_in = normed(embedded_h)
    def kv_copies(step):
        device = (my_req, my_cand, lax.rem(my_user + step, users))
        return [
            pltpu.make_async_remote_copy(
                src_ref=source,
                dst_ref=target.at[step - 1],
                send_sem=kv_send.at[2 * (step - 1) + part],
                recv_sem=kv_recv.at[2 * (step - 1) + part],
                device_id=device,
                device_id_type=MESH,
            )
            for part, (source, target) in enumerate(
                ((keys_own, keys_other), (values_own, values_other))
            )
        ]

    copies = [kv_copies(step) for step in range(1, users)]
    keys_own[...] = block(hist_in, 3).astype(BF16)
    for keys_copy, _ in copies:
        keys_copy.start()
    values_own[...] = block(hist_in, 1).astype(BF16)
    for _, values_copy in copies:
        values_copy.start()
    sends = [copy for pair in copies for copy in pair]
    queries[...] = block(hist_in, 2).astype(BF16)
    gate_u[...] = block(hist_in, 0)
    causal = one_hot(
        lax.broadcasted_iota(jnp.int32, (count_h, count_h), 0)
        >= lax.broadcasted_iota(jnp.int32, (count_h, count_h), 1)
    )
    half = count_h // 2
    attend(keys_own, values_own, causal[:half, :half], True, slice(0, half), slice(0, half))
    attend(keys_own, values_own, causal[half:], True, slice(half, count_h))
    for copy in sends:
        copy.wait_recv()
    for step in range(1, users):
        @pl.when(my_user >= step)
        def _():
            attend(keys_other.at[step - 1], values_other.at[step - 1], None, False)

    hist_out[...] = finish(embedded_h)

    gather((0, 3, 2, 1), slot_c, embedded_c, cap_c, cand_reply)
    cand_in = normed(embedded_c)
    queries[...] = block(cand_in, 2).astype(BF16)
    gate_u[...] = block(cand_in, 0)
    attend(keys_own, values_own, None, True)
    for step in range(1, users):
        attend(keys_other.at[step - 1], values_other.at[step - 1], None, False)
    cand_out[...] = finish(embedded_c)

    for copy in sends:
        copy.wait_send()

    @pl.loop(0, PLANES)
    def _(number):
        each_batch(
            served(number)[1], lambda count: replies_sent(number, count, *cand_reply).wait_send()
        )


def hand_out(hist_in, cand_in, hist_out, cand_out, out_sem):
    outward = [
        pltpu.make_async_copy(source, target, out_sem.at[place])
        for place, (source, target) in enumerate(((hist_in, hist_out), (cand_in, cand_out)))
    ]
    for copy in outward:
        copy.start()
    for copy in outward:
        copy.wait()


def per_device(sizes, table, hot_table, hot_ids, hist_ids, cand_ids, w_in, w_out, in_gain, attn_gain):
    reqs, cands, users = sizes
    owners = reqs * cands
    rows_owned, features = table.shape
    hot_count = hot_table.shape[0]
    count_h = hist_ids.shape[1]
    count_c = cand_ids.shape[1]
    cap_h = round_up(max(2, 2 * count_h // owners), 16)
    cap_c = round_up(max(2, 3 * count_c // (2 * owners)), 16)
    members = owners // PLANES
    group = 4 if members % 4 == 0 else 1
    pieces = 4
    vmem = pl.BlockSpec(memory_space=pltpu.VMEM)
    anywhere = pl.BlockSpec(memory_space=pl.ANY)
    dma = pltpu.SemaphoreType.DMA
    others = max(users - 1, 1)
    given = (
        table,
        hot_table,
        hot_ids[None],
        hist_ids,
        cand_ids,
        w_in[0],
        w_out[0],
        in_gain,
        attn_gain,
    )
    hist_out, cand_out = pl.pallas_call(
        functools.partial(kernel, (reqs, cands, users, cap_h, cap_c, group, pieces)),
        out_shape=(
            pltpu.VMEM((count_h, features), BF16),
            pltpu.VMEM((count_c, features), BF16),
        ),
        in_specs=[anywhere] * len(given),
        out_specs=(vmem, vmem),
        scratch_shapes=[
            pltpu.VMEM((1, hot_count), jnp.int32),
            pltpu.VMEM((1, count_h), jnp.int32),
            pltpu.VMEM((1, count_c), jnp.int32),
            pltpu.VMEM((1, features), F32),
            pltpu.VMEM((1, features), F32),
            pltpu.VMEM((3, rows_owned, features), BF16),
            pltpu.VMEM((hot_count, features), BF16),
            pltpu.VMEM((features, 4 * features), BF16),
            pltpu.VMEM((features, features), BF16),
            pltpu.VMEM((owners, 8, 128), jnp.int32),
            pltpu.VMEM((owners, 8, 128), jnp.int32),
            pltpu.VMEM((owners, cap_h, features), BF16),
            pltpu.VMEM((owners, cap_c, features), BF16),
            pltpu.VMEM((owners, cap_h, features), BF16),
            pltpu.VMEM((owners, cap_c, features), BF16),
            pltpu.VMEM((count_h, features), BF16),
            pltpu.VMEM((count_h, features), BF16),
            pltpu.VMEM((others, count_h, features), BF16),
            pltpu.VMEM((others, count_h, features), BF16),
            pltpu.VMEM((count_h, features), BF16),
            pltpu.VMEM((count_h, features), F32),
            pltpu.VMEM((count_h, features), F32),
            pltpu.VMEM((count_h, features), F32),
            pltpu.VMEM((count_c, features), F32),
            dma((len(given),)),
            dma((1,)),
            dma((PLANES,)),
            dma((PLANES,)),
            dma((PLANES,)),
            dma((PLANES,)),
            dma((PLANES,)),
            dma((2 * others,)),
            dma((2 * others,)),
            dma((2,)),
            dma((2 * pieces,)),
            dma((2 * others,)),
            dma((2 * others,)),
        ],
        compiler_params=pltpu.CompilerParams(
            collective_id=0, has_side_effects=True, vmem_limit_bytes=44 * 1024 * 1024
        ),
    )(*(pltpu.with_memory_space_constraint(array, pltpu.HBM) for array in given))
    hist_out, cand_out = pl.pallas_call(
        hand_out,
        out_shape=(
            jax.ShapeDtypeStruct((count_h, features), BF16),
            jax.ShapeDtypeStruct((count_c, features), BF16),
        ),
        in_specs=[vmem, vmem],
        out_specs=(anywhere, anywhere),
        scratch_shapes=[dma((2,))],
        compiler_params=pltpu.CompilerParams(vmem_limit_bytes=16 * 1024 * 1024),
    )(hist_out, cand_out)
    return hist_out[None], cand_out[None]


def solution(mesh):
    sizes = tuple(mesh.shape[name] for name in ("req", "cand", "user"))
    in_specs = (
        P(("req", "cand"), None),
        P(),
        P(),
        P(("req", "cand"), "user"),
        P(("req", "cand"), "user"),
        P(),
        P(),
        P(),
        P(),
    )
    out_specs = (P(("req", "cand"), "user", None), P(("req", "cand"), "user", None))
    return jax.shard_map(
        functools.partial(per_device, sizes),
        mesh=mesh,
        in_specs=in_specs,
        out_specs=out_specs,
        check_vma=False,
    )
```
